32 devices in a mesh: row: 4 (over x, core), col: 8 (over z, y).
Axes of the slice: x: 2, y: 2, z: 4, core: 2. Of those that a mesh axis runs over, the one named last changes fastest.
Arguments:
- tiles: bfloat16 [4, 8, 128, 128, 128], P('row', 'col')
- tile_row: int32 [4, 8, 128], P('row', 'col'), may hold values from 0 to 15, as said below
- tile_col: int32 [4, 8, 128], P('row', 'col'), may hold values from 0 to 15
- tile_count: int32 [4, 8], P('row', 'col'), may hold values from 1 to 128, as said below
- sinogram: float32 [4, 2048, 128], P('row', 'col')
Outputs:
- volume: float32 [8, 2048, 128], P('col', 'row')
- residual: float32 [4, 2048, 128], P('row', 'col')
The draws below stay inside these ranges and needn't reach their ends.
Inputs may be any that keep to these rules, and one draw needn't show every extreme that they name: Within one block the pairs (tile_row, tile_col) of all 128 slots are distinct. Slots 0 to tile_count - 1 of a block are live, the rest are ignored; some block has all 128 slots live in every draw.
All inputs are finite; a program needn't handle non-finite values.
Results may differ from the reference program's by a relative error of at most 0.015.
Values may be sent and summed in bfloat16 or wider, within the bound.
A program may use at most 64 MiB of HBM per device.

```python
import jax
import jax.numpy as jnp
from jax import lax

TILE = 128
RT = 16
VT = 16
TMAX = 128
FRAMES = 128
ITERS = 4
RAYS = 2048
VOX = 2048
N_ROW = 4
N_COL = 8


def tile_pairs(key):
    keys = jax.random.split(jax.random.fold_in(key, 7), N_ROW * N_COL)

    def shuffled(single):
        return jax.random.permutation(single, jnp.arange(RT * VT, dtype=jnp.int32))
    order = jax.vmap(shuffled)(keys)[:, :TMAX]
    rows = (order // VT).reshape(N_ROW, N_COL, TMAX).astype(jnp.int32)
    cols = (order % VT).reshape(N_ROW, N_COL, TMAX).astype(jnp.int32)
    return (rows, cols)


def draw_tile_row(key, part):
    return tile_pairs(key)[0]


def draw_tile_col(key, part):
    return tile_pairs(key)[1]


def draw_tile_count(key, part):
    base = TMAX // 8 + jax.random.randint(jax.random.fold_in(key, 3), (N_ROW * N_COL,), 0, TMAX // 2 + 1)
    base = jnp.maximum(base, 1)
    fullest = jax.random.randint(jax.random.fold_in(key, 5), (), 0, N_ROW * N_COL)
    base = jnp.where(jnp.arange(N_ROW * N_COL, dtype=jnp.int32) == fullest, TMAX, base)
    return base.reshape(N_ROW, N_COL).astype(jnp.int32)


def draw_tiles(key, part):
    shape = (N_ROW, N_COL, TMAX, TILE, TILE)
    place = lax_index(shape)
    rising = 3.0 ** (place / max(N_ROW * N_COL - 1, 1))
    fan = (TILE * N_COL * TMAX // (2 * RT)) ** (-0.5)
    values = jax.random.normal(jax.random.fold_in(key, 11), shape, jnp.float32)
    return (values * rising * fan).astype(jnp.bfloat16)


def lax_index(shape):
    first = jax.lax.broadcasted_iota(jnp.float32, shape, 0)
    second = jax.lax.broadcasted_iota(jnp.float32, shape, 1)
    return first * N_COL + second


def draw_sinogram(key, part):
    shape = (N_ROW, RAYS, FRAMES)
    ray = jax.lax.broadcasted_iota(jnp.float32, shape, 0) * RAYS + jax.lax.broadcasted_iota(jnp.float32, shape, 1)
    rising = 3.0 ** (ray / (N_ROW * RAYS - 1))
    values = jnp.clip(jax.random.normal(jax.random.fold_in(key, 17), shape, jnp.float32), -6.0, 6.0)
    return values * rising * 0.25


def setup_inputs(seed: int = 0) -> dict:
    key_of = jax.random.split(jax.random.key(seed), 6)
    return {
        "tiles": draw_tiles(jax.random.fold_in(key_of[5], 71), 0),
        "tile_row": draw_tile_row(jax.random.fold_in(key_of[5], 71), 0),
        "tile_col": draw_tile_col(jax.random.fold_in(key_of[5], 71), 0),
        "tile_count": draw_tile_count(jax.random.fold_in(key_of[5], 71), 0),
        "sinogram": draw_sinogram(jax.random.fold_in(key_of[5], 71), 0),
    }


def tile_pick(table, index):
    return lax.optimization_barrier(jnp.take(table, index, axis=0))


def forward_block(blocks, rows_index, cols_index, count, voxel_tiles):
    picked = tile_pick(voxel_tiles, cols_index)
    products = jnp.einsum("tij,tjk->tik", blocks.astype(jnp.float32), picked.astype(jnp.float32))
    live = jnp.arange(TMAX, dtype=jnp.int32) < count
    select = ((rows_index[None, :] == jnp.arange(RT, dtype=jnp.int32)[:, None]) & live[None, :]).astype(jnp.float32)
    return jnp.einsum("ut,tik->uik", select, products, precision=lax.Precision.HIGHEST)


def backward_block(blocks, rows_index, cols_index, count, ray_tiles):
    picked = tile_pick(ray_tiles, rows_index)
    products = jnp.einsum("tji,tjk->tik", blocks.astype(jnp.float32), picked.astype(jnp.float32))
    live = jnp.arange(TMAX, dtype=jnp.int32) < count
    select = ((cols_index[None, :] == jnp.arange(VT, dtype=jnp.int32)[:, None]) & live[None, :]).astype(jnp.float32)
    return jnp.einsum("ut,tik->uik", select, products, precision=lax.Precision.HIGHEST)


def reference(tiles, tile_row, tile_col, tile_count, sinogram):
    blocks_all = tiles.reshape(N_ROW * N_COL, TMAX, TILE, TILE)
    rows_all = tile_row.reshape(N_ROW * N_COL, TMAX)
    cols_all = tile_col.reshape(N_ROW * N_COL, TMAX)
    counts_all = tile_count.reshape(N_ROW * N_COL)
    devices = jnp.arange(N_ROW * N_COL, dtype=jnp.int32)

    def apply_forward(direction):
        voxel_tiles = direction.astype(jnp.bfloat16).reshape(N_COL, VT, TILE, FRAMES)

        def single(device):
            return forward_block(blocks_all[device], rows_all[device], cols_all[device],
                                 counts_all[device], voxel_tiles[device % N_COL])

        parts = lax.map(single, devices)
        return parts.reshape(N_ROW, N_COL, RAYS, FRAMES).sum(axis=1)

    def apply_backward(field):
        ray_tiles = field.astype(jnp.bfloat16).reshape(N_ROW, RT, TILE, FRAMES)

        def single(device):
            return backward_block(blocks_all[device], rows_all[device], cols_all[device],
                                  counts_all[device], ray_tiles[device // N_COL])

        parts = lax.map(single, devices)
        return parts.reshape(N_ROW, N_COL, VOX, FRAMES).sum(axis=0)

    volume = jnp.zeros((N_COL, VOX, FRAMES), jnp.float32)
    residual = sinogram
    search = apply_backward(residual)
    gamma = jnp.sum(search * search, axis=(0, 1))
    direction = search
    for step in range(ITERS):
        image = apply_forward(direction)
        alpha = gamma / jnp.sum(image * image, axis=(0, 1))
        volume = volume + alpha * direction
        residual = residual - alpha * image
        if step + 1 < ITERS:
            search = apply_backward(residual)
            fresh = jnp.sum(search * search, axis=(0, 1))
            direction = search + (fresh / gamma) * direction
            gamma = fresh
    return volume, residual
```

```python
import functools

import jax
import jax.numpy as jnp
from jax import lax
from jax.experimental import pallas as pl
from jax.experimental.pallas import tpu as pltpu
from jax.sharding import PartitionSpec as P

RT = 16
VT = 16
ITERS = 4
CORES = 2
MESH = pl.DeviceIdType.MESH
F32 = jnp.float32
BF16 = jnp.bfloat16


def inner_size(n):
    size = 1
    while size * 2 * size * 2 <= n and n % (size * 2) == 0:
        size *= 2
    return size


def spread_kernel(rows_ref, cols_ref, count_ref, tiles_ref, dense_ref, flipped_ref):
    tile = tiles_ref.shape[1]
    dense_ref[...] = jnp.zeros_like(dense_ref)
    flipped_ref[...] = jnp.zeros_like(flipped_ref)

    def place(t, carry):
        r = pl.multiple_of(rows_ref[t] * tile, tile)
        c = pl.multiple_of(cols_ref[t] * tile, tile)
        block = tiles_ref[t]
        dense_ref[pl.ds(r, tile), pl.ds(c, tile)] = block
        flipped_ref[pl.ds(c, tile), pl.ds(r, tile)] = block.T
        return carry

    lax.fori_loop(0, count_ref[0], place, 0)


class Axis:
    def __init__(self, name, n, n_in, chunk, refs):
        self.name, self.n, self.n_in, self.n_out, self.chunk = name, n, n_in, n // n_in, chunk
        self.near_out, self.near_in, self.far_out, self.far_in, self.norm_in = refs[:5]
        (self.near_ss, self.near_rs, self.far_ss, self.far_rs, self.out_ss, self.out_rs,
         self.in_ss, self.in_rs, self.norm_ss, self.norm_rs) = refs[5:]
        self.me = lax.axis_index(name)
        self.o, self.i = self.me // n_in, lax.rem(self.me, n_in)

    def index(self, e, d):
        return lax.rem(self.o + e + self.n_out, self.n_out) * self.n_in + lax.rem(self.i + d + self.n_in, self.n_in)

    def rows(self, index):
        return pl.ds(pl.multiple_of(index * self.chunk, self.chunk), self.chunk)

    def send(self, src, dst, ss, rs, index):
        copy = pltpu.make_async_remote_copy(
            src_ref=src, dst_ref=dst, send_sem=ss, recv_sem=rs,
            device_id={self.name: index}, device_id_type=MESH,
        )
        copy.start()
        return copy

    def outer_order(self):
        return sorted(range(1, self.n_out), key=lambda e: -min(e, self.n_out - e)) + [0]

    def reduce_scatter(self, matrix, full):
        def piece(index):
            return jnp.dot(matrix[self.rows(index), :], full[...], preferred_element_type=F32)

        copies = []
        near = {}
        for e in self.outer_order():
            for d in range(1, self.n_in):
                self.near_out[d - 1, e] = piece(self.index(e, d)).astype(BF16)
                near[e, d] = self.send(
                    self.near_out.at[d - 1, e], self.near_in.at[d - 1, e],
                    self.near_ss.at[d - 1, e], self.near_rs.at[d - 1, e], self.index(0, d))
        far = {}
        total = None
        for e in self.outer_order():
            total = piece(self.index(e, 0))
            for d in range(1, self.n_in):
                near[e, d].wait_recv()
                total += self.near_in[d - 1, e].astype(F32)
            if e:
                self.far_out[e - 1] = total.astype(BF16)
                far[e] = self.send(
                    self.far_out.at[e - 1], self.far_in.at[e - 1],
                    self.far_ss.at[e - 1], self.far_rs.at[e - 1], self.index(e, 0))
        for e in far:
            far[e].wait_recv()
            total += self.far_in[e - 1].astype(F32)
        for copy in list(near.values()) + list(far.values()):
            copy.wait_send()
        return total

    def all_gather(self, value, full):
        full[self.rows(self.me), :] = value.astype(BF16)
        mine = full.at[self.rows(self.me), :]
        far, near = {}, {}
        for e in self.outer_order()[:-1]:
            far[e] = self.send(mine, mine, self.out_ss.at[e - 1], self.out_rs.at[e - 1], self.index(e, 0))
        for d in range(1, self.n_in):
            near[0, d] = self.send(mine, mine, self.in_ss.at[d - 1, 0], self.in_rs.at[d - 1, 0], self.index(0, d))
        for e in reversed(self.outer_order()[:-1]):
            far[e].wait_recv()
            theirs = full.at[self.rows(self.index(-e, 0)), :]
            for d in range(1, self.n_in):
                near[e, d] = self.send(
                    theirs, theirs, self.in_ss.at[d - 1, e], self.in_rs.at[d - 1, e], self.index(0, d))
        for copy in near.values():
            copy.wait_recv()
        for copy in list(near.values()) + list(far.values()):
            copy.wait_send()

    def peer(self, d):
        return lax.rem(self.me + d, self.n)

    def norm_send(self, value, which):
        self.norm_in[which, 0] = jnp.broadcast_to(value, self.norm_in.shape[2:])
        return [
            self.send(self.norm_in.at[which, 0], self.norm_in.at[which, d],
                      self.norm_ss.at[which, d - 1], self.norm_rs.at[which, d - 1], self.peer(d))
            for d in range(1, self.n)
        ]

    def norm_wait(self, which):
        for d in range(1, self.n):
            pltpu.make_async_remote_copy(
                src_ref=self.norm_in.at[which, 0], dst_ref=self.norm_in.at[which, d],
                send_sem=self.norm_ss.at[which, d - 1], recv_sem=self.norm_rs.at[which, d - 1],
                device_id={self.name: self.peer(d)}, device_id_type=MESH,
            ).wait()
        total = self.norm_in[which, 0]
        for d in range(1, self.n):
            total += self.norm_in[which, d]
        return total[0:1, :]


def squares(ref, step):
    total = None
    for at in range(0, ref.shape[0], step):
        part = ref[at:at + step, :].astype(F32)
        part = jnp.sum(part * part, axis=0, keepdims=True)
        total = part if total is None else total + part
    return total


def cgls_kernel(sizes, dense_hbm, flipped_hbm, sino_ref, volume_ref, residual_ref, dense, flipped, rays, voxels,
                search, direction, image, gamma, load_sem, *refs):
    n_row, n_col, col_in = sizes
    half = len(refs) // 2
    row = Axis("row", n_row, CORES, search.shape[0], refs[:half])
    col = Axis("col", n_col, col_in, image.shape[0], refs[half:])

    loads = [
        pltpu.make_async_copy(flipped_hbm, flipped, load_sem.at[0]),
        pltpu.make_async_copy(dense_hbm, dense, load_sem.at[1]),
    ]
    for load in loads:
        load.start()

    barrier = pltpu.get_barrier_semaphore()
    for axis in (row, col):
        for d in range(1, axis.n):
            pl.semaphore_signal(barrier, inc=1, device_id={axis.name: axis.peer(d)}, device_id_type=MESH)
    pl.semaphore_wait(barrier, n_row + n_col - 2)

    col.all_gather(sino_ref[...], rays)
    residual_ref[...] = sino_ref[...]
    volume_ref[...] = jnp.zeros_like(volume_ref)
    direction[...] = jnp.zeros_like(direction)
    image[...] = jnp.zeros_like(image)
    gamma[...] = jnp.ones_like(gamma)
    for load in loads:
        load.wait()

    def iteration(k, carry):
        search[...] = row.reduce_scatter(flipped, rays)
        row.all_gather(search[...], voxels)
        col.norm_send(squares(voxels, 256), 0)
        forth = col.reduce_scatter(dense, voxels)
        fresh = col.norm_wait(0)
        beta = jnp.where(k > 0, fresh / gamma[...], jnp.zeros_like(fresh))
        gamma[...] = fresh
        image[...] = forth + beta * image[...]
        col.norm_send(squares(image, image.shape[0]), 1)
        direction[...] = search[...] + beta * direction[...]
        row.norm_send(col.norm_wait(1), 0)
        alpha = fresh / row.norm_wait(0)
        residual_ref[...] -= alpha * image[...]

        @pl.when(k + 1 < ITERS)
        def _():
            col.all_gather(residual_ref[...], rays)

        volume_ref[...] += alpha * direction[...]
        return carry

    lax.fori_loop(0, ITERS, iteration, 0)


def axis_scratch(n, n_in, chunk, frames):
    n_out = n // n_in
    dma = pltpu.SemaphoreType.DMA
    near, far = (max(n_in - 1, 1), n_out), (max(n_out - 1, 1),)
    return [
        pltpu.VMEM(near + (chunk, frames), BF16),
        pltpu.VMEM(near + (chunk, frames), BF16),
        pltpu.VMEM(far + (chunk, frames), BF16),
        pltpu.VMEM(far + (chunk, frames), BF16),
        pltpu.VMEM((2, n, 8, frames), F32),
        dma(near), dma(near), dma(far), dma(far), dma(far), dma(far), dma(near), dma(near),
        dma((2, n - 1)), dma((2, n - 1)),
    ]


def local(n_row, n_col, tiles, tile_row, tile_col, tile_count, sinogram):
    tile, frames = tiles.shape[3], sinogram.shape[2]
    n_rays, n_vox = RT * tile, VT * tile
    vmem = pl.BlockSpec(memory_space=pltpu.VMEM)
    smem = pl.BlockSpec(memory_space=pltpu.SMEM)
    dense, flipped = pl.pallas_call(
        spread_kernel,
        out_shape=(
            jax.ShapeDtypeStruct((n_rays, n_vox), BF16),
            jax.ShapeDtypeStruct((n_vox, n_rays), BF16),
        ),
        in_specs=[smem, smem, smem, vmem],
        out_specs=(vmem, vmem),
        compiler_params=pltpu.CompilerParams(vmem_limit_bytes=40 * 1024 * 1024),
        name="spread",
    )(tile_row[0, 0], tile_col[0, 0], tile_count[0], tiles[0, 0])

    col_in = inner_size(n_col)
    vox_piece, ray_piece = n_vox // n_row, n_rays // n_col
    hbm = pl.BlockSpec(memory_space=pl.ANY)
    volume, residual = pl.pallas_call(
        functools.partial(cgls_kernel, (n_row, n_col, col_in)),
        out_shape=(
            jax.ShapeDtypeStruct((vox_piece, frames), F32),
            jax.ShapeDtypeStruct((ray_piece, frames), F32),
        ),
        in_specs=[hbm, hbm, vmem],
        out_specs=(vmem, vmem),
        scratch_shapes=[
            pltpu.VMEM((n_rays, n_vox), BF16),
            pltpu.VMEM((n_vox, n_rays), BF16),
            pltpu.VMEM((n_rays, frames), BF16),
            pltpu.VMEM((n_vox, frames), BF16),
            pltpu.VMEM((vox_piece, frames), F32),
            pltpu.VMEM((vox_piece, frames), F32),
            pltpu.VMEM((ray_piece, frames), F32),
            pltpu.VMEM((1, frames), F32),
            pltpu.SemaphoreType.DMA((2,)),
        ]
        + axis_scratch(n_row, CORES, vox_piece, frames)
        + axis_scratch(n_col, col_in, ray_piece, frames),
        compiler_params=pltpu.CompilerParams(
            collective_id=0, has_side_effects=True, vmem_limit_bytes=40 * 1024 * 1024
        ),
        name="cgls",
    )(dense, flipped, sinogram[0])
    return volume[None], residual[None]


def solution(mesh):
    return jax.shard_map(
        functools.partial(local, mesh.shape["row"], mesh.shape["col"]),
        mesh=mesh,
        in_specs=(
            P("row", "col", None, None, None),
            P("row", "col", None),
            P("row", "col", None),
            P("row", "col"),
            P("row", "col", None),
        ),
        out_specs=(P("col", "row", None), P("row", "col", None)),
        check_vma=False,
    )
```

```python
import functools

import jax
import jax.numpy as jnp
from jax import lax
from jax.experimental import pallas as pl
from jax.experimental.pallas import tpu as pltpu
from jax.sharding import PartitionSpec as P

RT = 16
VT = 16
ITERS = 4
CORES = 2
MESH = pl.DeviceIdType.MESH
F32 = jnp.float32
BF16 = jnp.bfloat16


def inner_size(n):
    size = 1
    while size * 2 * size * 2 <= n and n % (size * 2) == 0:
        size *= 2
    return size


def build(slot_ref, tiles, dense, flipped, start, stop):
    tile = tiles.shape[1]
    group = 4

    def place(step, carry):
        for j in range(group):
            at = step * group + j
            r = pl.multiple_of(at // VT * tile, tile)
            c = pl.multiple_of(lax.rem(at, VT) * tile, tile)
            block = tiles[slot_ref[at]]
            dense[pl.ds(r, tile), pl.ds(c, tile)] = block
            flipped[pl.ds(c, tile), pl.ds(r, tile)] = block.T
        return carry

    lax.fori_loop(start // group, stop // group, place, 0)


class Axis:
    def __init__(self, name, n, n_in, chunk, refs):
        self.name, self.n, self.n_in, self.n_out, self.chunk = name, n, n_in, n // n_in, chunk
        self.near_out, self.near_in, self.far_out, self.far_in, self.norm_in = refs[:5]
        (self.near_ss, self.near_rs, self.far_ss, self.far_rs, self.out_ss, self.out_rs,
         self.in_ss, self.in_rs, self.norm_ss, self.norm_rs) = refs[5:]
        self.me = lax.axis_index(name)
        self.o, self.i = self.me // n_in, lax.rem(self.me, n_in)

    def index(self, e, d):
        return lax.rem(self.o + e + self.n_out, self.n_out) * self.n_in + lax.rem(self.i + d + self.n_in, self.n_in)

    def rows(self, index):
        return pl.ds(pl.multiple_of(index * self.chunk, self.chunk), self.chunk)

    def send(self, src, dst, ss, rs, index):
        copy = pltpu.make_async_remote_copy(
            src_ref=src, dst_ref=dst, send_sem=ss, recv_sem=rs,
            device_id={self.name: index}, device_id_type=MESH,
        )
        copy.start()
        return copy

    def outer_order(self):
        return sorted(range(1, self.n_out), key=lambda e: -min(e, self.n_out - e)) + [0]

    def reduce_scatter(self, matrix, full):
        def piece(index):
            return jnp.dot(matrix[self.rows(index), :], full[...], preferred_element_type=F32)

        copies = []
        near = {}
        for e in self.outer_order():
            for d in range(1, self.n_in):
                self.near_out[d - 1, e] = piece(self.index(e, d)).astype(BF16)
                near[e, d] = self.send(
                    self.near_out.at[d - 1, e], self.near_in.at[d - 1, e],
                    self.near_ss.at[d - 1, e], self.near_rs.at[d - 1, e], self.index(0, d))
        far = {}
        total = None
        for e in self.outer_order():
            total = piece(self.index(e, 0))
            for d in range(1, self.n_in):
                near[e, d].wait_recv()
                total += self.near_in[d - 1, e].astype(F32)
            if e:
                self.far_out[e - 1] = total.astype(BF16)
                far[e] = self.send(
                    self.far_out.at[e - 1], self.far_in.at[e - 1],
                    self.far_ss.at[e - 1], self.far_rs.at[e - 1], self.index(e, 0))
        for e in far:
            far[e].wait_recv()
            total += self.far_in[e - 1].astype(F32)
        for copy in list(near.values()) + list(far.values()):
            copy.wait_send()
        return total

    def all_gather(self, value, full, between=lambda step: None):
        full[self.rows(self.me), :] = value.astype(BF16)
        mine = full.at[self.rows(self.me), :]
        far, near = {}, {}
        for e in self.outer_order()[:-1]:
            far[e] = self.send(mine, mine, self.out_ss.at[e - 1], self.out_rs.at[e - 1], self.index(e, 0))
        for d in range(1, self.n_in):
            near[0, d] = self.send(mine, mine, self.in_ss.at[d - 1, 0], self.in_rs.at[d - 1, 0], self.index(0, d))
        between(0)
        for step, e in enumerate(reversed(self.outer_order()[:-1])):
            far[e].wait_recv()
            theirs = full.at[self.rows(self.index(-e, 0)), :]
            for d in range(1, self.n_in):
                near[e, d] = self.send(
                    theirs, theirs, self.in_ss.at[d - 1, e], self.in_rs.at[d - 1, e], self.index(0, d))
            between(step + 1)
        for copy in near.values():
            copy.wait_recv()
        for copy in list(near.values()) + list(far.values()):
            copy.wait_send()

    def peer(self, d):
        return lax.rem(self.me + d, self.n)

    def norm_send(self, value, which):
        self.norm_in[which, 0] = jnp.broadcast_to(value, self.norm_in.shape[2:])
        return [
            self.send(self.norm_in.at[which, 0], self.norm_in.at[which, d],
                      self.norm_ss.at[which, d - 1], self.norm_rs.at[which, d - 1], self.peer(d))
            for d in range(1, self.n)
        ]

    def norm_wait(self, which):
        for d in range(1, self.n):
            pltpu.make_async_remote_copy(
                src_ref=self.norm_in.at[which, 0], dst_ref=self.norm_in.at[which, d],
                send_sem=self.norm_ss.at[which, d - 1], recv_sem=self.norm_rs.at[which, d - 1],
                device_id={self.name: self.peer(d)}, device_id_type=MESH,
            ).wait()
        total = self.norm_in[which, 0]
        for d in range(1, self.n):
            total += self.norm_in[which, d]
        return total[0:1, :]


def squares(ref, step):
    total = None
    for at in range(0, ref.shape[0], step):
        part = ref[at:at + step, :].astype(F32)
        part = jnp.sum(part * part, axis=0, keepdims=True)
        total = part if total is None else total + part
    return total


def cgls_kernel(sizes, slot_ref, tiles_hbm, sino_ref, volume_ref, residual_ref, tiles, dense, flipped, rays, voxels,
                images, held, search, direction, image, gamma, per_alpha, load_sem, *refs):
    n_row, n_col, col_in = sizes
    half = len(refs) // 2
    row = Axis("row", n_row, CORES, search.shape[0], refs[:half])
    col = Axis("col", n_col, col_in, image.shape[0], refs[half:])

    slots = tiles_hbm.shape[0]
    load = pltpu.make_async_copy(tiles_hbm, tiles.at[pl.ds(0, slots)], load_sem)
    load.start()
    tiles[slots] = jnp.zeros(tiles.shape[1:], tiles.dtype)

    barrier = pltpu.get_barrier_semaphore()
    for axis in (row, col):
        for d in range(1, axis.n):
            pl.semaphore_signal(barrier, inc=1, device_id={axis.name: axis.peer(d)}, device_id_type=MESH)
    pl.semaphore_wait(barrier, n_row + n_col - 2)

    share = RT * VT // col.n_out

    def build_share(step):
        if step == 0:
            load.wait()
        build(slot_ref, tiles, dense, flipped, step * share, (step + 1) * share)

    col.all_gather(sino_ref[...], rays, build_share)
    held[...] = rays[...].astype(F32)
    residual_ref[...] = sino_ref[...]
    volume_ref[...] = jnp.zeros_like(volume_ref)
    direction[...] = jnp.zeros_like(direction)
    image[...] = jnp.zeros_like(image)
    gamma[...] = jnp.ones_like(gamma)
    per_alpha[...] = jnp.zeros_like(per_alpha)

    def iteration(k, carry):
        search[...] = row.reduce_scatter(flipped, rays)
        row.all_gather(search[...], voxels)
        col.norm_send(squares(voxels, 256), 0)
        forth = col.reduce_scatter(dense, voxels)
        fresh = col.norm_wait(0)
        beta = jnp.where(k > 0, fresh / gamma[...], jnp.zeros_like(fresh))
        gamma[...] = fresh
        image[...] = forth + beta * image[...]
        col.norm_send(squares(image, image.shape[0]), 1)

        @pl.when(k + 1 < ITERS)
        def _():
            def norm_on(step):
                if step == col.n_out - 1:
                    row.norm_send(col.norm_wait(1), 0)

            drift = held[col.rows(col.me), :] - residual_ref[...]
            col.all_gather(image[...] + drift * per_alpha[...], images, norm_on)

        @pl.when(k + 1 == ITERS)
        def _():
            row.norm_send(col.norm_wait(1), 0)

        direction[...] = search[...] + beta * direction[...]
        energy = row.norm_wait(0)
        alpha = fresh / energy
        per_alpha[...] = energy / fresh

        @pl.when(k + 1 < ITERS)
        def _():
            held[...] -= alpha * images[...].astype(F32)
            rays[...] = held[...].astype(BF16)

        residual_ref[...] -= alpha * image[...]
        volume_ref[...] += alpha * direction[...]
        return carry

    lax.fori_loop(0, ITERS, iteration, 0)


def axis_scratch(n, n_in, chunk, frames):
    n_out = n // n_in
    dma = pltpu.SemaphoreType.DMA
    near, far = (max(n_in - 1, 1), n_out), (max(n_out - 1, 1),)
    return [
        pltpu.VMEM(near + (chunk, frames), BF16),
        pltpu.VMEM(near + (chunk, frames), BF16),
        pltpu.VMEM(far + (chunk, frames), BF16),
        pltpu.VMEM(far + (chunk, frames), BF16),
        pltpu.VMEM((2, n, 8, frames), F32),
        dma(near), dma(near), dma(far), dma(far), dma(far), dma(far), dma(near), dma(near),
        dma((2, n - 1)), dma((2, n - 1)),
    ]


def local(n_row, n_col, tiles, tile_row, tile_col, tile_count, sinogram):
    tile, frames = tiles.shape[3], sinogram.shape[2]
    n_rays, n_vox = RT * tile, VT * tile
    vmem = pl.BlockSpec(memory_space=pltpu.VMEM)
    smem = pl.BlockSpec(memory_space=pltpu.SMEM)
    slots = tiles.shape[2]
    slot = jnp.arange(slots, dtype=jnp.int32)
    place = tile_row[0, 0] * VT + tile_col[0, 0]
    match = (place[None, :] == jnp.arange(RT * VT, dtype=jnp.int32)[:, None]) & (slot[None, :] < tile_count[0, 0])
    slot_of = jnp.min(jnp.where(match, slot[None, :], slots), axis=1)

    col_in = inner_size(n_col)
    vox_piece, ray_piece = n_vox // n_row, n_rays // n_col
    hbm = pl.BlockSpec(memory_space=pl.ANY)
    volume, residual = pl.pallas_call(
        functools.partial(cgls_kernel, (n_row, n_col, col_in)),
        out_shape=(
            jax.ShapeDtypeStruct((vox_piece, frames), F32),
            jax.ShapeDtypeStruct((ray_piece, frames), F32),
        ),
        in_specs=[smem, hbm, vmem],
        out_specs=(vmem, vmem),
        scratch_shapes=[
            pltpu.VMEM((slots + 1, tile, tile), BF16),
            pltpu.VMEM((n_rays, n_vox), BF16),
            pltpu.VMEM((n_vox, n_rays), BF16),
            pltpu.VMEM((n_rays, frames), BF16),
            pltpu.VMEM((n_vox, frames), BF16),
            pltpu.VMEM((n_rays, frames), BF16),
            pltpu.VMEM((n_rays, frames), F32),
            pltpu.VMEM((vox_piece, frames), F32),
            pltpu.VMEM((vox_piece, frames), F32),
            pltpu.VMEM((ray_piece, frames), F32),
            pltpu.VMEM((1, frames), F32),
            pltpu.VMEM((1, frames), F32),
            pltpu.SemaphoreType.DMA,
        ]
        + axis_scratch(n_row, CORES, vox_piece, frames)
        + axis_scratch(n_col, col_in, ray_piece, frames),
        compiler_params=pltpu.CompilerParams(
            collective_id=0, has_side_effects=True, vmem_limit_bytes=62 * 1024 * 1024
        ),
        name="cgls",
    )(slot_of, tiles[0, 0], sinogram[0])
    return volume[None], residual[None]


def solution(mesh):
    return jax.shard_map(
        functools.partial(local, mesh.shape["row"], mesh.shape["col"]),
        mesh=mesh,
        in_specs=(
            P("row", "col", None, None, None),
            P("row", "col", None),
            P("row", "col", None),
            P("row", "col"),
            P("row", "col", None),
        ),
        out_specs=(P("col", "row", None), P("row", "col", None)),
        check_vma=False,
    )
```
